256 devices in a mesh: expert: 8 (over y, core), shard: 32 (over x, z).
Axes of the slice: x: 4, y: 4, z: 8, core: 2. Of those that a mesh axis runs over, the one named last changes fastest.
Arguments:
- params: float32 [3, 8, 6144, 256], P(None, 'expert', 'shard'), may hold values from -3 to 3
- grads: float32 [3, 8, 6144, 256], P(None, 'expert', 'shard')
- moment: float32 [3, 8, 6144, 256], P(None, 'expert', 'shard'), may hold values from -0.6 to 0.6
- second: float32 [3, 8, 64], P(None, 'expert'), may hold values from 0.002 to 0.2
- step: int32 [1], replicated, may hold values from 1 to 8
- block_map: int32 [256], replicated, may hold values from 0 to 63, never falling along the last dimension, each value on 1 to 8 neighbouring positions
Outputs:
- new_weights: bfloat16 [3, 8, 6144, 256], P(None, 'expert')
- new_moment: float32 [3, 8, 6144, 256], P(None, 'expert', 'shard')
- new_second: float32 [3, 8, 64], P(None, 'expert')
The draws below stay inside these ranges and needn't reach their ends.
Inputs may be any that keep to these rules, and one draw needn't show every extreme that they name: `block_map`: every block holds at least one neuron and at most 8.
All inputs are finite; a program needn't handle non-finite values.
Results may differ from the reference program's by a relative error of at most 0.001.
Values may be sent and summed in bfloat16 or wider, within the bound.
No kernel may reach another device: no remote copies, remote signals or barrier semaphores. Data moves between devices by JAX's collectives and lax.ppermute only.
A program may use at most 64 MiB of HBM per device.

```python
import math
import jax
import jax.numpy as jnp
import numpy as np
from jax import lax

D = 6144
NEUR = 256
NBLK = 64
EXPERTS = 8


def draw_grads(key, part):
    keys = jax.random.split(key, 4)
    row_place = jnp.arange(D, dtype=jnp.float32) / D
    expert_place = jnp.arange(EXPERTS, dtype=jnp.float32) / EXPERTS
    noise = jax.random.normal(keys[0], (3, EXPERTS, D, NEUR), jnp.float32)
    row_scale = jnp.power(10.0, 0.5 * row_place + 0.5 * jax.random.uniform(keys[1], (D,), jnp.float32))
    column_scale = jnp.power(10.0, jax.random.uniform(keys[2], (NEUR,), jnp.float32))
    expert_scale = jnp.power(10.0, 0.25 * expert_place + 0.25 * jax.random.uniform(keys[3], (EXPERTS,), jnp.float32))
    return noise * row_scale[None, None, :, None] * column_scale[None, None, None, :] * expert_scale[None, :, None, None]


def block_scale(stream_key, dims, cuts, low, top_value):
    level, own = 1.0, jax.random.fold_in(stream_key, 6)
    for position, blocks in cuts:
        heights = jnp.exp(jax.random.uniform(jax.random.fold_in(own, position), (blocks,), jnp.float32, low / len(cuts), top_value / len(cuts)))
        level = level * jnp.repeat(heights, dims[position] // blocks).reshape([-1 if axis == position else 1 for axis in range(len(dims))])
    return level


def length_profile(count, total, reach, skew):
    loads = [(1 << 20) // math.isqrt(rank ** skew) + 1 for rank in range(2, count + 1)]
    rest, holding = total - reach - (count - 1), [1] * (count - 1)
    while rest > 0:
        candidates = [i for i in range(count - 1) if holding[i] < reach]
        pool, remaining = sum([loads[i] for i in candidates]), rest
        for i in candidates:
            addition = min(reach - holding[i], max(1, remaining * loads[i] // pool), rest)
            holding[i] = holding[i] + addition
            rest = rest - addition
    return np.array([reach] + holding)


def uneven(key, amount, total, reach, skew):
    if amount == 2:
        one = jax.random.randint(key, (), max(1, total - reach), min(reach, total - 1) + 1)
        return jnp.stack([one, total - one])
    sizes = jnp.asarray(length_profile(amount, total, reach, skew), jnp.int32)
    couples = (amount - 1) // 2
    donor, receiver = sizes[1:1 + 2 * couples:2], sizes[2:2 + 2 * couples:2]
    margin = jnp.minimum(donor - 1, reach - receiver)
    moved = jax.random.randint(jax.random.fold_in(key, 1), (couples,), 0, 1 << 20) % (margin + 1)
    sizes = sizes.at[1:1 + 2 * couples:2].set(donor - moved).at[2:2 + 2 * couples:2].set(receiver + moved)
    return sizes[jax.random.permutation(jax.random.fold_in(key, 2), amount)]


def centred(rng, shape, width, reach, pieces=(), kind=jnp.bfloat16):
    level = block_scale(rng, shape, pieces, -0.22, 0.18) if pieces else 1.0
    drawn = jax.random.normal(rng, shape, jnp.float32) * width * level
    return jnp.minimum(jnp.maximum(drawn, -reach), reach).astype(kind)


def setup_inputs(seed: int = 0) -> dict:
    key_list = jax.random.split(jax.random.key(seed), 7)
    return {
        "params": centred(key_list[0], (3, EXPERTS, D, NEUR), 0.5, 3.0, ((1, 8), (2, 32)), jnp.float32),
        "grads": draw_grads(jax.random.fold_in(key_list[6], 71), 0),
        "moment": centred(key_list[2], (3, EXPERTS, D, NEUR), 0.1, 0.6, ((1, 8), (2, 32)), jnp.float32),
        "second": jnp.clip(jnp.exp(math.log(0.2) - 4.6051702 * jax.random.uniform(key_list[3], (3, EXPERTS, NBLK), jnp.float32) ** block_scale(key_list[3], (3, EXPERTS, NBLK), ((1, 8),), -0.2, 0.2)), 0.002, 0.2),
        "step": jax.random.randint(key_list[4], (1,), 1, 9).astype(jnp.int32),
        "block_map": jnp.searchsorted(jnp.cumsum(uneven(key_list[5], NBLK, NEUR, 8, 1)), jnp.arange(NEUR), side="right").astype(jnp.int32),
    }


LEARN_RATE = 0.05
DECAY_WEIGHT = 0.1
BETA_FIRST = 0.9
BETA_SECOND = 0.95
epsilon = 1e-08

def reference(params, grads, moment, second, step, block_map):
    member_table = (block_map[:, None] == jnp.arange(NBLK, dtype=jnp.int32)[None, :]).astype(jnp.float32)
    members = lax.optimization_barrier(jnp.sum(member_table, axis=0))
    squares = lax.optimization_barrier(jnp.sum(grads * grads, axis=2))
    block_sums = jnp.einsum('ken,nb->keb', squares, member_table, precision=lax.Precision.HIGHEST)
    total = jnp.sum(block_sums)
    limit = math.sqrt(3 * EXPERTS * D * NEUR)
    clip = jnp.minimum(1.0, limit / (jnp.sqrt(total) + 1e-06))
    new_second = BETA_SECOND * second + (1.0 - BETA_SECOND) * clip * clip * block_sums / (D * members)
    new_moment = BETA_FIRST * moment + (1.0 - BETA_FIRST) * clip * grads
    step_value = step[0].astype(jnp.float32)
    first_fix = 1.0 - jnp.power(jnp.float32(BETA_FIRST), step_value)
    second_fix = 1.0 - jnp.power(jnp.float32(BETA_SECOND), step_value)
    divisor = jnp.sqrt(new_second / second_fix) + epsilon
    by_neuron = jnp.einsum('keb,nb->ken', divisor, member_table, precision=lax.Precision.HIGHEST)
    updated = params * (1.0 - LEARN_RATE * DECAY_WEIGHT) - LEARN_RATE * (new_moment / first_fix) / by_neuron[:, :, None, :]
    return (updated.astype(jnp.bfloat16), new_moment, new_second)
```

```python
import math

import jax
import jax.numpy as jnp
from jax import lax
from jax.experimental import pallas as pl
from jax.experimental.pallas import tpu as pltpu
from jax.sharding import PartitionSpec as P


LEARN_RATE = 0.05
DECAY_WEIGHT = 0.1
BETA_FIRST = 0.9
BETA_SECOND = 0.95
epsilon = 1e-08

NX, NZ = 4, 8
ROWS = 192
CUT = 80


def copy_for_each(x, axis):
    length = lax.axis_size(axis)
    return lax.all_to_all(jnp.broadcast_to(x[None], (length, *x.shape)), axis, 0, 0, tiled=True)


def taken_together(x, axis):
    everything = copy_for_each(x, axis)
    return jnp.sum(everything, axis=0)


def shift(value, dx, dz):
    pairs = [
        (x * NZ + z, (x + dx) % NX * NZ + (z + dz) % NZ) for x in range(NX) for z in range(NZ)
    ]
    return lax.ppermute(value, "shard", pairs)


def assemble(pieces, places, out):
    def kernel(*refs):
        *ins, _, dst, sem = refs
        me = lax.axis_index("shard")
        x, z = me // NZ, me % NZ
        copies = []
        for ref, spots in zip(ins, places):
            for g, (dx, dz, off) in enumerate(spots):
                source = (x + dx) % NX * NZ + (z + dz) % NZ
                start = pl.multiple_of(source * ROWS + off, 8)
                copies.append(
                    pltpu.make_async_copy(
                        ref.at[pl.ds(3 * g, 3)],
                        dst.at[:, 0, pl.ds(start, ref.shape[1]), :],
                        sem,
                    )
                )
        for copy in copies:
            copy.start()
        for copy in copies:
            copy.wait()

    first = out is None
    shape = jax.ShapeDtypeStruct((3, 1, ROWS * NX * NZ, 256), jnp.bfloat16)
    if first:
        def body(*refs):
            *ins, dst, sem = refs
            kernel(*ins, None, dst, sem)

        args, aliases = list(pieces), {}
    else:
        body, args, aliases = kernel, [*pieces, out], {len(pieces): 0}
    return pl.pallas_call(
        body,
        out_shape=shape,
        in_specs=[pl.BlockSpec(memory_space=pl.ANY)] * len(args),
        out_specs=pl.BlockSpec(memory_space=pl.ANY),
        scratch_shapes=[pltpu.SemaphoreType.DMA],
        input_output_aliases=aliases,
        compiler_params=pltpu.CompilerParams(vmem_limit_bytes=4 * 2**20),
        name="assemble",
    )(*args)


def gather(own):
    pieces, places = [], []

    def put(piece, spots):
        pieces.append(piece)
        places.append(spots)

    half = ROWS // 2
    low = own[:, :CUT]
    put(own, [(0, 0, 0)])
    up, down = {0: own}, {0: own}
    up[1] = shift(up[0], 0, 1)
    down[1] = shift(down[0], 0, -1)
    xm = shift(low, 1, 0)
    xp = shift(low, -1, 0)
    xo = shift(low, 2, 0)
    for k in (2, 3):
        up[k] = shift(up[k - 1], 0, 1)
        down[k] = shift(down[k - 1], 0, -1)
    up4 = shift(up[3][:, :half], 0, 1)
    down4 = shift(down[3][:, half:], 0, -1)
    for k in (1, 2, 3):
        put(up[k], [(0, -k, 0)])
        put(down[k], [(0, k, 0)])
    put(up4, [(0, 4, 0)])
    put(down4, [(0, 4, half)])
    put(xm, [(-1, 0, 0)])
    put(xp, [(1, 0, 0)])
    put(xo, [(2, 0, 0)])
    u = d = jnp.concatenate([xm, xp, xo], axis=0)
    xs = (-1, 1, 2)
    for k in (1, 2, 3):
        u = shift(u, 0, 1)
        d = shift(d, 0, -1)
        put(u, [(x, -k, 0) for x in xs])
        put(d, [(x, k, 0) for x in xs])
    u = shift(u[:, : CUT // 2], 0, 1)
    d = shift(d[:, CUT // 2 :], 0, -1)
    put(u, [(x, 4, 0) for x in xs])
    put(d, [(x, 4, CUT // 2) for x in xs])
    rest = (ROWS - CUT) // 2
    one = jnp.concatenate([p[:, CUT:] for p in (own, up[1], down[1])], axis=0)
    four = jnp.concatenate([up4[:, CUT:], down4], axis=1)
    two = jnp.concatenate([*(p[:, CUT:] for p in (up[2], down[2], up[3], down[3])), four], axis=0)
    for group, zs in ((one, (0, -1, 1)), (two, (-2, 2, -3, 3, 4))):
        u = shift(group, 1, 0)
        d = shift(group, -1, 0)
        put(u, [(-1, z, CUT) for z in zs])
        put(d, [(1, z, CUT) for z in zs])
        u = shift(u[:, :rest], 1, 0)
        d = shift(d[:, rest:], -1, 0)
        put(u, [(2, z, CUT) for z in zs])
        put(d, [(2, z, CUT + rest) for z in zs])
    return assemble(pieces, places, None)


def body(params, grads, moment, second, step, block_map):
    blocks = second.shape[2]
    member_table = (block_map[:, None] == jnp.arange(blocks, dtype=jnp.int32)[None, :]).astype(
        jnp.float32
    )
    members = jnp.sum(member_table, axis=0)
    width = grads.shape[2] * lax.axis_size("shard")
    squares = jnp.sum(grads * grads, axis=2)
    local_sums = jnp.einsum("ken,nb->keb", squares, member_table, precision=lax.Precision.HIGHEST)
    block_sums = taken_together(local_sums, "shard")
    total = taken_together(jnp.sum(block_sums), "expert")
    limit = math.sqrt(3 * lax.axis_size("expert") * grads.shape[1] * width * grads.shape[3])
    clip = jnp.minimum(1.0, limit / (jnp.sqrt(total) + 1e-06))
    new_second = BETA_SECOND * second + (1.0 - BETA_SECOND) * clip * clip * block_sums / (
        width * members
    )
    new_moment = BETA_FIRST * moment + (1.0 - BETA_FIRST) * clip * grads
    step_value = step[0].astype(jnp.float32)
    first_fix = 1.0 - jnp.power(jnp.float32(BETA_FIRST), step_value)
    second_fix = 1.0 - jnp.power(jnp.float32(BETA_SECOND), step_value)
    divisor = jnp.sqrt(new_second / second_fix) + epsilon
    by_neuron = jnp.einsum("keb,nb->ken", divisor, member_table, precision=lax.Precision.HIGHEST)
    updated = (
        params * (1.0 - LEARN_RATE * DECAY_WEIGHT)
        - LEARN_RATE * (new_moment / first_fix) / by_neuron[:, :, None, :]
    )
    new_weights = gather(updated.astype(jnp.bfloat16)[:, 0])
    return (new_weights, new_moment, new_second)


def solution(mesh):
    placed = (
        P(None, "expert", "shard", None),
        P(None, "expert", "shard", None),
        P(None, "expert", "shard", None),
        P(None, "expert", None),
        P(),
        P(),
    )

    return jax.shard_map(
        body,
        mesh=mesh,
        in_specs=placed,
        out_specs=(
            P(None, "expert", None, None),
            P(None, "expert", "shard", None),
            P(None, "expert", None),
        ),
        check_vma=False,
    )
```
